128 devices in a mesh: prob: 1, feat: 128 (over z, y, x, core).
Axes of the slice: x: 4, y: 4, z: 4, core: 2. Of those that a mesh axis runs over, the one named last changes fastest.
Arguments:
- design: bfloat16 [16384, 32768], P('prob', 'feat')
- coef_init: float32 [32768, 3], P(('prob', 'feat'))
- targets: float32 [16384, 3], P('prob')
- step_sizes: float32 [32768], P(('prob', 'feat'))
Outputs:
- output 1: float32 [32768, 3], P(('prob', 'feat'))
- output 2: float32 [16384, 3], P('prob')
All inputs are finite; a program needn't handle non-finite values.
Results may differ from the reference program's by a relative error of at most 0.00440094.
Values are sent between devices in bfloat16 or wider.
A program may use at most 1 GiB of HBM per device.

```python
import jax
import jax.numpy as jnp
from jax import lax

SAMPLES = 16384
FEAT_DEV = 256
GROUP_SIZE = 128
TARGETS = 3
SWEEPS = 6
FACTORS = 4

FEATURES = FEAT_DEV * GROUP_SIZE
COMBINE_WEIGHT = 0.8
LASSO_WEIGHT = 0.3 * GROUP_SIZE / FEATURES ** 0.5


def setup_inputs(seed: int = 0, part: int = 0) -> dict:
    part_key = jax.random.fold_in(jax.random.key(seed), part)
    draw_keys = jax.random.split(part_key, 9)
    factor_rows = jax.random.normal(draw_keys[0], (SAMPLES, FACTORS), jnp.float32)
    loadings = jax.random.normal(draw_keys[1], (FACTORS, FEATURES), jnp.float32) * (0.5 / FEAT_DEV) ** 0.5

    def draw_block(block_index):
        noise_x = jax.random.normal(jax.random.fold_in(draw_keys[2], block_index), (SAMPLES, FEAT_DEV), jnp.float32)
        load_block = lax.dynamic_slice_in_dim(loadings, block_index * FEAT_DEV, FEAT_DEV, 1)
        x_block = (jnp.dot(factor_rows, load_block) + noise_x).astype(jnp.bfloat16)
        col_sq = jnp.sum(jnp.square(x_block.astype(jnp.float32)), axis=0)
        return x_block, col_sq

    x_blocks, col_sq = lax.map(draw_block, jnp.arange(GROUP_SIZE))
    design = jnp.transpose(x_blocks, (1, 0, 2)).reshape(SAMPLES, FEATURES)
    step_scale = jax.random.uniform(draw_keys[3], (FEATURES,), jnp.float32, 0.5, 1.0)
    step_sizes = step_scale * SAMPLES / (GROUP_SIZE * col_sq.reshape(FEATURES))
    support = jax.random.bernoulli(draw_keys[4], 0.125, (FEATURES, TARGETS)).astype(jnp.float32)
    true_weights = jax.random.normal(draw_keys[5], (FEATURES, TARGETS), jnp.float32) * support * (4.0 / FEATURES) ** 0.5
    factor_weights = jax.random.normal(draw_keys[6], (FACTORS, TARGETS), jnp.float32) * FACTORS ** -0.5
    noise_y = jax.random.normal(draw_keys[7], (SAMPLES, TARGETS), jnp.float32)
    signal = jnp.dot(design, true_weights.astype(jnp.bfloat16), preferred_element_type=jnp.float32)
    targets = jnp.dot(factor_rows, factor_weights) + signal + 0.5 * noise_y
    coef_init = jax.random.normal(draw_keys[8], (FEATURES, TARGETS), jnp.float32) * FEATURES ** -0.5
    return {'design': design, 'coef_init': coef_init, 'targets': targets, 'step_sizes': step_sizes}


def reference(design, coef_init, targets, step_sizes):
    x_blocks = jnp.transpose(design.reshape(SAMPLES, GROUP_SIZE, FEAT_DEV), (1, 0, 2))
    step_col = step_sizes[:, None]
    thresholds = step_col * LASSO_WEIGHT

    def block_sum(values):
        value_blocks = values.astype(jnp.bfloat16).reshape(GROUP_SIZE, FEAT_DEV, TARGETS)

        def add_block(running, operands):
            x_block, v_block = operands
            product = jnp.dot(x_block, v_block, preferred_element_type=jnp.float32).astype(jnp.bfloat16)
            return running + product.astype(jnp.float32), None

        running, _ = lax.scan(add_block, jnp.zeros((SAMPLES, TARGETS), jnp.float32), (x_blocks, value_blocks))
        return running

    residual = targets - block_sum(coef_init)

    def sweep(carry, _):
        weights, residual = carry
        gradient = lax.dot_general(design, residual.astype(jnp.bfloat16), (((0,), (0,)), ((), ())), preferred_element_type=jnp.float32) / SAMPLES
        stepped = weights + step_col * gradient
        shrunk = jnp.sign(stepped) * jnp.maximum(jnp.abs(stepped) - thresholds, 0.0)
        change = shrunk - weights
        weights = weights + COMBINE_WEIGHT * change
        residual = residual - COMBINE_WEIGHT * block_sum(change)
        return (weights, residual), None

    (weights, residual), _ = lax.scan(sweep, (coef_init, residual), None, length=SWEEPS)
    return (weights, residual)
```

```python
import jax
import jax.numpy as jnp
from jax import lax
from jax.experimental import pallas as pl
from jax.experimental.pallas import tpu as pltpu
from jax.sharding import PartitionSpec as P

SWEEPS = 6
COMBINE_WEIGHT = 0.8
ROWS = 4
PIECE = 128


def solution(mesh):
    group = mesh.shape['feat']

    def body(x_hbm, w_in, y_hbm, eta_in, w_out, r_out,
             x_v, w_s, dw_s, u_send, u_recv, r_send, r_all, r_own, g_s,
             x_sem, y_sem, us_sem, ur_sem, rs_sem, rr_sem, fs_sem, fr_sem):
        me = lax.axis_index('feat')
        samples = x_hbm.shape[0]
        blk = x_hbm.shape[1]
        features = blk * group
        lasso_weight = 0.3 * group / features ** 0.5
        n_tiles = samples // 256
        tiles_per_load = n_tiles // x_sem.shape[0]
        load_rows = tiles_per_load * 256

        def x_load(i):
            rows = pl.ds(i * load_rows, load_rows)
            return pltpu.make_async_copy(x_hbm.at[rows], x_v.at[rows], x_sem.at[i])

        for i in range(x_sem.shape[0]):
            x_load(i).start()
        y_load = pltpu.make_async_copy(y_hbm.at[:, pl.ds(pl.multiple_of(me * PIECE, PIECE), PIECE)], r_own.at[pl.ds(0, 3)], y_sem)
        r_own[...] = jnp.zeros_like(r_own)

        barrier = pltpu.get_barrier_semaphore()

        def greet(i, carry):
            pl.semaphore_signal(barrier, inc=1, device_id={'feat': lax.rem(me + i, group)}, device_id_type=pl.DeviceIdType.MESH)
            return carry

        lax.fori_loop(1, group, greet, 0)

        w_s[...] = jnp.zeros_like(w_s)
        w_s[pl.ds(0, 3), :] = w_in[...]
        dw_s[...] = w_s[...].astype(jnp.bfloat16)
        step = eta_in[...]
        thr = step * lasso_weight

        def u_tile(c):
            xt = x_v[pl.ds(pl.multiple_of(c * 256, 256), 256), :]
            u = lax.dot_general(dw_s[...], xt, (((1,), (1,)), ((), ())), preferred_element_type=jnp.float32)
            ub = u.astype(jnp.bfloat16)
            u_send[2 * c] = ub[:ROWS, :PIECE]
            u_send[2 * c + 1] = ub[:ROWS, PIECE:]

        def u_copy(dest):
            return pltpu.make_async_remote_copy(
                src_ref=u_send.at[dest], dst_ref=u_recv.at[me], send_sem=us_sem, recv_sem=ur_sem,
                device_id={'feat': dest}, device_id_type=pl.DeviceIdType.MESH)

        def u_all():
            return pltpu.make_async_remote_copy(
                src_ref=u_send.at[pl.ds(0, group - 1)], dst_ref=u_recv.at[pl.ds(0, group - 1)], send_sem=us_sem, recv_sem=ur_sem,
                device_id={'feat': me}, device_id_type=pl.DeviceIdType.MESH)

        def r_copy(dest):
            return pltpu.make_async_remote_copy(
                src_ref=r_send, dst_ref=r_all.at[me], send_sem=rs_sem, recv_sem=rr_sem,
                device_id={'feat': dest}, device_id_type=pl.DeviceIdType.MESH)

        def r_gather():
            return pltpu.make_async_remote_copy(
                src_ref=r_all.at[pl.ds(0, group - 1)], dst_ref=r_all.at[pl.ds(0, group - 1)], send_sem=rs_sem, recv_sem=rr_sem,
                device_id={'feat': me}, device_id_type=pl.DeviceIdType.MESH)

        def send(copy):
            def one(i, carry):
                copy(lax.rem(me + i, group)).start()
                return carry
            lax.fori_loop(1, group, one, 0)

        def scatter_and_sum():
            send(u_copy)
            u_recv[me] = u_send[me]
            u_all().wait_recv()
            u_all().wait_send()
            acc = jnp.zeros((ROWS, PIECE), jnp.float32)
            for s in range(0, group, 16):
                acc = acc + jnp.sum(u_recv[pl.ds(s, 16)].astype(jnp.float32), axis=0)
            return acc

        y_load.start()
        for i in range(x_sem.shape[0]):
            x_load(i).wait()
            def tiles(c, carry, i=i):
                u_tile(i * tiles_per_load + c)
                return carry
            lax.fori_loop(0, tiles_per_load, tiles, 0, unroll=True)
        pl.semaphore_wait(barrier, group - 1)
        y_load.wait()
        r_own[...] = r_own[...] - scatter_and_sum()

        def sweep(t, carry):
            rb = r_own[...].astype(jnp.bfloat16)
            r_send[...] = rb
            r_all[me] = rb
            send(r_copy)
            r_gather().wait_recv()
            r_gather().wait_send()
            g = jnp.zeros((ROWS, blk), jnp.float32)
            for c in range(n_tiles):
                lhs = jnp.concatenate([r_all[2 * c], r_all[2 * c + 1]], axis=1)
                g = g + jnp.dot(lhs, x_v[pl.ds(c * 256, 256), :], preferred_element_type=jnp.float32)
            w = w_s[pl.ds(0, ROWS), :]
            v = w + step * (g / samples)
            v = jnp.maximum(v - thr, 0.0) + jnp.minimum(v + thr, 0.0)
            dw = v - w
            w_s[pl.ds(0, ROWS), :] = w + COMBINE_WEIGHT * dw
            dw_s[pl.ds(0, ROWS), :] = dw.astype(jnp.bfloat16)

            def tiles(c, carry):
                u_tile(c)
                return carry
            lax.fori_loop(0, n_tiles, tiles, 0, unroll=8)
            r_own[...] = r_own[...] - COMBINE_WEIGHT * scatter_and_sum()
            return carry

        lax.fori_loop(0, SWEEPS, sweep, 0)
        w_out[...] = w_s[pl.ds(0, 3), :]

        mine = pl.ds(pl.multiple_of(me * PIECE, PIECE), PIECE)
        r_out[:, mine] = r_own[...]

        def f_copy(dest):
            return pltpu.make_async_remote_copy(
                src_ref=r_own, dst_ref=r_out.at[:, mine], send_sem=fs_sem, recv_sem=fr_sem,
                device_id={'feat': dest}, device_id_type=pl.DeviceIdType.MESH)
        send(f_copy)
        done = pltpu.make_async_remote_copy(
            src_ref=r_out.at[:, pl.ds(0, (group - 1) * PIECE)], dst_ref=r_out.at[:, pl.ds(0, (group - 1) * PIECE)], send_sem=fs_sem, recv_sem=fr_sem,
            device_id={'feat': me}, device_id_type=pl.DeviceIdType.MESH)
        done.wait_recv()
        done.wait_send()

    def local_run(x_local, coef_local, targets_local, step_local):
        samples, blk = x_local.shape
        vmem = pl.BlockSpec(memory_space=pltpu.VMEM)
        hbm = pl.BlockSpec(memory_space=pltpu.HBM)
        w_t, r_t = pl.pallas_call(
            body,
            out_shape=(jax.ShapeDtypeStruct((3, blk), jnp.float32), jax.ShapeDtypeStruct((ROWS, samples), jnp.float32)),
            in_specs=[hbm, vmem, hbm, vmem],
            out_specs=(vmem, vmem),
            scratch_shapes=[
                pltpu.VMEM((samples, blk), jnp.bfloat16),
                pltpu.VMEM((8, blk), jnp.float32),
                pltpu.VMEM((8, blk), jnp.bfloat16),
                pltpu.VMEM((group, ROWS, PIECE), jnp.bfloat16),
                pltpu.VMEM((group, ROWS, PIECE), jnp.bfloat16),
                pltpu.VMEM((ROWS, PIECE), jnp.bfloat16),
                pltpu.VMEM((group, ROWS, PIECE), jnp.bfloat16),
                pltpu.VMEM((ROWS, PIECE), jnp.float32),
                pltpu.VMEM((8, blk), jnp.float32),
                pltpu.SemaphoreType.DMA((8,)),
                pltpu.SemaphoreType.DMA,
                pltpu.SemaphoreType.DMA, pltpu.SemaphoreType.DMA,
                pltpu.SemaphoreType.DMA, pltpu.SemaphoreType.DMA,
                pltpu.SemaphoreType.DMA, pltpu.SemaphoreType.DMA,
            ],
            compiler_params=pltpu.CompilerParams(collective_id=0, has_side_effects=True, vmem_limit_bytes=48 * 1024 * 1024),
        )(x_local, coef_local.T, targets_local.T, step_local[None, :])
        return w_t.T, r_t[:3].T

    return jax.shard_map(local_run, mesh=mesh, in_specs=(P('prob', 'feat'), P(('prob', 'feat'), None), P('prob', None), P(('prob', 'feat'))), out_specs=(P(('prob', 'feat'), None), P('prob', None)), check_vma=False)
```
